32 devices in a mesh: gx: 4 (over y, x), gy: 8 (over z, core).
Axes of the slice: x: 2, y: 2, z: 4, core: 2. Of those that a mesh axis runs over, the one named last changes fastest.
Arguments:
- tiles: bfloat16 [64, 24, 128, 128], P('gx', 'gy'), may hold values from 0.0099487305 to 1
- tile_cols: int32 [64, 24], P('gx', 'gy'), may hold values from 0 to 7
- row_counts: int32 [64, 8], P('gx', 'gy'), may hold values from 0 to 3
- start_block: bfloat16 [8192, 128], P('gx'), may hold values from -6 to 6
Outputs:
- vectors: bfloat16 [8192, 128], P(('gx', 'gy'))
- col_scales: float32 [2, 128], replicated
The draws below stay inside these ranges and needn't reach their ends.
Inputs may be any that keep to these rules, and one draw needn't show every extreme that they name: `tile_cols`: a column tile inside the slot's block of columns. `row_counts`: slots at or past the count are ignored.
All inputs are finite; a program needn't handle non-finite values.
Results may differ from the reference program's by a relative error of at most 0.0065.
Values may be sent and summed in bfloat16 or wider, within the bound.
A program may use at most 64 MiB of HBM per device.

```python
import math
import jax
import jax.numpy as jnp
import numpy as np
from jax import lax

TILE = 128
K = 128
RT = 16
MAXT = 3
ROWTILES = 64
CT = 8
NODES = 8192
N_GX = 4
N_GY = 8


def with_ends(values, stream_key, low, high):
    extent = values.shape
    index_at = [jax.random.randint(jax.random.fold_in(stream_key, axis), (), 0, extent[axis]) for axis in range(len(extent))]
    values = values.at[tuple(index_at)].set(low)
    longest = extent.index(max(extent))
    index_at[longest] = (index_at[longest] + 1) % extent[longest]
    return values.at[tuple(index_at)].set(high)


def steps_of(stream_key, extent, pieces, low, top_value):
    def one(dim, shards_of):
        draws = jax.random.uniform(jax.random.fold_in(jax.random.fold_in(stream_key, 6), dim), (shards_of,), jnp.float32, low / len(pieces), top_value / len(pieces))
        return jnp.repeat(jnp.exp(draws), extent[dim] // shards_of).reshape((-1,) + (1,) * (len(extent) - dim - 1))

    loudness = one(*pieces[0])
    for cut in pieces[1:]:
        loudness = loudness * one(*cut)
    return loudness


def rank_table(amount, skew):
    weights = [(1 << 20) // math.isqrt(grade ** skew) + 1 for grade in range(1, amount + 1)]
    scale = 1 + sum(weights) // (1 << 30)
    return np.cumsum(np.array([max(1, weight // scale) for weight in weights]))


def ranked(own_key, extent, amount, lean):
    table = rank_table(amount, lean)
    lot = jax.random.randint(jax.random.fold_in(own_key, 1), extent, 0, int(table[amount - 1]))
    standing = jnp.searchsorted(jnp.asarray(table, jnp.int32), lot, side="right")
    return jax.random.permutation(jax.random.fold_in(own_key, 2), amount)[standing].astype(jnp.int32)


def centred(rng, extent, deviation, most, cuts=(), kind=jnp.bfloat16):
    gain = steps_of(rng, extent, cuts, -0.22, 0.18) if cuts else 1.0
    entries = jax.random.normal(rng, extent, jnp.float32) * deviation * gain
    return jnp.minimum(jnp.maximum(entries, -most), most).astype(kind)


def setup_inputs(seed: int = 0) -> dict:
    seeds = jax.random.split(jax.random.key(seed), 5)
    return {
        "tiles": jnp.clip(jnp.exp(math.log(1.0) - 4.61031033 * jax.random.uniform(seeds[0], (ROWTILES, N_GY * MAXT, TILE, TILE), jnp.float32) ** steps_of(seeds[0], (ROWTILES, N_GY * MAXT, TILE, TILE), ((0, 4), (1, 8)), -0.2, 0.2)), 0.0099487305, 1.0).astype(jnp.bfloat16),
        "tile_cols": with_ends(jax.random.randint(seeds[1], (ROWTILES, N_GY * MAXT), 0, CT), jax.random.fold_in(seeds[1], 1), 0, CT - 1).astype(jnp.int32),
        "row_counts": with_ends(ranked(seeds[2], (ROWTILES, N_GY), MAXT + 1, 2), jax.random.fold_in(seeds[2], 3), 0, MAXT).astype(jnp.int32),
        "start_block": centred(seeds[3], (NODES, K), 1.0, 6.0, ((0, 4),)),
    }


def apply_graph(tiles, tile_cols, row_counts, upd):
    row_tiles = tiles.shape[0]
    col_tiles = RT * N_GX // N_GY
    slots = jnp.arange(MAXT)

    def one_block(index, total):
        index = jnp.asarray(index).astype(jnp.int32)
        block_tiles = lax.dynamic_slice_in_dim(tiles, (index * MAXT).astype(jnp.int32), MAXT, 1).astype(jnp.float32)
        block_cols = lax.dynamic_slice_in_dim(tile_cols, (index * MAXT).astype(jnp.int32), MAXT, 1)
        counts = lax.dynamic_slice_in_dim(row_counts, index, 1, 1)
        masks = (slots[None, :] < counts).astype(jnp.float32)
        column = lax.dynamic_slice_in_dim(upd, (index * col_tiles * TILE).astype(jnp.int32), col_tiles * TILE, 0)
        column = column.reshape(col_tiles, TILE, K).astype(jnp.float32)
        picked = column[block_cols] * masks[:, :, None, None]
        return total + jnp.einsum('rsab,rsbk->rak', block_tiles, picked)
    total = lax.fori_loop(0, N_GY, one_block, jnp.zeros((row_tiles, TILE, K), jnp.float32))
    return total.reshape(row_tiles * TILE, K)

def row_degree(tiles, row_counts):
    slots = jnp.arange(MAXT)

    def one_block(index, total):
        index = jnp.asarray(index).astype(jnp.int32)
        block_tiles = lax.dynamic_slice_in_dim(tiles, (index * MAXT).astype(jnp.int32), MAXT, 1).astype(jnp.float32)
        counts = lax.dynamic_slice_in_dim(row_counts, index, 1, 1)
        masks = (slots[None, :] < counts).astype(jnp.float32)
        return total + jnp.einsum('rsab,rs->ra', block_tiles, masks)
    total = lax.fori_loop(0, N_GY, one_block, jnp.zeros((tiles.shape[0], TILE), jnp.float32))
    return 1.0 + total.reshape(-1)

def reference(tiles, tile_cols, row_counts, start_block):
    nodes = tiles.shape[0] * TILE
    scale = 1.0 / jnp.sqrt(row_degree(tiles, row_counts))
    upd = (scale[:, None] * start_block.astype(jnp.float32)).astype(jnp.bfloat16)
    scales = []
    vectors = upd
    for step in range(2):
        partial_value = apply_graph(tiles, tile_cols, row_counts, upd)
        mixed = scale[:, None] * (partial_value + upd.astype(jnp.float32))
        spread = jnp.sqrt(lax.optimization_barrier(jnp.sum(mixed * mixed, axis=0)) / nodes + 1e-06)
        scales.append(spread)
        normed = mixed / spread
        if step == 0:
            upd = (scale[:, None] * normed).astype(jnp.bfloat16)
        else:
            vectors = normed.astype(jnp.bfloat16)
    return (vectors, jnp.stack(scales))
```

```python
import functools
import jax
import jax.numpy as jnp
from jax import lax
from jax.experimental import pallas as pl
from jax.experimental.pallas import tpu as pltpu
from jax.sharding import PartitionSpec as P

MESH = pl.DeviceIdType.MESH
LOADS = 4


def wait(ref, sem):
    pltpu.make_async_copy(ref, ref, sem).wait()


def kernel(
    groups,
    blocks,
    tiles_hbm,
    start_hbm,
    cols,
    counts,
    out,
    sums_out,
    tiles,
    sbuf,
    ubuf,
    vbuf,
    scol,
    sshare,
    rs,
    deg_col,
    deg_share,
    psend,
    precv,
    acc,
    csend,
    clow,
    chigh,
    p2send,
    p2recv,
    r2send,
    r2recv,
    last,
    sq,
    tsem,
    ssend,
    srecv,
    dcs,
    dcr,
    dss,
    dsr,
    psd,
    prc,
    csd,
    clr,
    chr_,
    vsend,
    vrecv,
    p2s,
    p2r,
    r2s,
    r2r,
    qs,
    qr,
):
    row_tiles, slots, side, _ = tiles.shape
    width = acc.shape[1]
    depth = acc.shape[0]
    col_tiles = depth // side
    share = out.shape[0]
    floors = blocks // 2
    total = groups * blocks
    nodes = groups * row_tiles * side
    piece = min(side, share)
    pieces = share // piece
    share_tiles = max(1, share // side)
    square = groups == 4

    i = lax.axis_index("gx")
    j = lax.axis_index("gy")
    z = lax.div(j, 2)
    c = lax.rem(j, 2)
    me = i * blocks + j
    root = i == z
    if square:
        x, y = lax.rem(i, 2), lax.div(i, 2)
        across_x = y * 2 + 1 - x
        across_y = (1 - y) * 2 + x
        off_x = x != lax.rem(z, 2)
        off_y = y != lax.div(z, 2)
        only_x = jnp.logical_and(off_x, jnp.logical_not(off_y))
        only_y = jnp.logical_and(off_y, jnp.logical_not(off_x))
        fan = 2
    else:
        fan = groups - 1

    def rows(ref, t):
        if len(ref.shape) == 3:
            return ref.at[t]
        return ref.at[pl.ds(t * side, side)]

    def remote(src, dst, send, recv, gx, gy):
        return pltpu.make_async_remote_copy(
            src_ref=src,
            dst_ref=dst,
            send_sem=send,
            recv_sem=recv,
            device_id=(gx, gy),
            device_id_type=MESH,
        )

    def fan_out(buf, send, recv, t):
        for p in range(fan):
            if square:
                target = (across_x, across_y)[p]
            else:
                target = lax.rem(i + p + 1, groups)
            remote(rows(buf, t), rows(buf, t), send.at[p, t], recv.at[t], target, j).start()

    def pass_on(buf, send, recv, t):
        if square:
            cond, target = ((only_x, across_y), (only_y, across_x))[t % 2]

            @pl.when(cond)
            def _():
                remote(rows(buf, t), rows(buf, t), send.at[0, t], recv.at[t], target, j).start()

    def fan_done(buf, send):
        @pl.when(root)
        def _():
            for t in range(col_tiles):
                for p in range(fan):
                    wait(rows(buf, t), send.at[p, t])

        if square:
            for parity, cond in ((0, only_x), (1, only_y)):

                @pl.when(cond)
                def _():
                    for t in range(parity, col_tiles, 2):
                        wait(rows(buf, t), send.at[0, t])

    step = row_tiles // LOADS
    loads = [
        pltpu.make_async_copy(
            tiles_hbm.at[pl.ds(n * step, step)], tiles.at[pl.ds(n * step, step)], tsem.at[n]
        )
        for n in range(LOADS)
    ]
    barrier = pltpu.get_barrier_semaphore()

    @pl.loop(1, total)
    def _(k):
        other = lax.rem(me + k, total)
        pl.semaphore_signal(
            barrier,
            inc=1,
            device_id=(lax.div(other, blocks), lax.rem(other, blocks)),
            device_id_type=MESH,
        )

    @pl.when(root)
    def _():
        for t in range(col_tiles):
            pltpu.make_async_copy(
                start_hbm.at[pl.ds(c * depth + t * side, side)], rows(sbuf, t), srecv.at[t]
            ).start()

    for load in loads:
        load.start()
    ubuf[col_tiles] = jnp.zeros((side, width), ubuf.dtype)
    vbuf[col_tiles] = jnp.zeros((side, width), vbuf.dtype)
    pl.semaphore_wait(barrier, total - 1)

    @pl.when(root)
    def _():
        for t in range(col_tiles):
            wait(rows(sbuf, t), srecv.at[t])
            fan_out(sbuf, ssend, srecv, t)

    ones = jnp.ones((8, side), jnp.bfloat16)
    for r in range(row_tiles):
        if r % step == 0:
            loads[r // step].wait()
        count = counts[r, 0]
        row = jnp.zeros((8, side), jnp.float32)
        for s in range(slots):
            part = lax.dot_general(
                ones, tiles[r, s], (((1,), (1,)), ((), ())), preferred_element_type=jnp.float32
            )
            row = row + jnp.clip(count - s, 0, 1).astype(jnp.float32) * part
        rs[r] = row[0:1]

    for h in range(2):
        source = rs.at[pl.ds(h * col_tiles, col_tiles)]
        for n in range(groups):
            target = lax.rem(i + n, groups)
            gy = 2 * i + h
            slot = deg_col.at[j]
            mine = jnp.logical_and(n == 0, gy == j)

            @pl.when(jnp.logical_not(mine))
            def _():
                remote(source, slot, dcs.at[h * groups + n], dcr.at[j], target, gy).start()

            @pl.when(mine)
            def _():
                pltpu.make_async_copy(source, slot, dcr.at[j]).start()

    def share_of(gy):
        return rs.at[pl.ds(lax.div(gy * share, side), share_tiles)]

    for n in range(1, blocks):
        gy = lax.rem(j + n, blocks)
        remote(share_of(gy), deg_share.at[j], dss.at[n], dsr.at[j], i, gy).start()
    pltpu.make_async_copy(share_of(j), deg_share.at[j], dsr.at[j]).start()

    @pl.when(jnp.logical_not(root))
    def _():
        for t in range(col_tiles):
            wait(rows(sbuf, t), srecv.at[t])
            pass_on(sbuf, ssend, srecv, t)

    for n in range(blocks):
        wait(deg_col.at[n], dcr.at[n])

    def upright(degree):
        scale = 1.0 / jnp.sqrt(1.0 + degree)
        return jnp.transpose(jnp.broadcast_to(scale, (side, side)))

    for t in range(col_tiles):
        degree = deg_col[0, t]
        for n in range(1, blocks):
            degree = degree + deg_col[n, t]
        scale = upright(degree)[:, :1]
        scale = jnp.broadcast_to(scale, (side, width))
        scol[pl.ds(t * side, side)] = scale
        ubuf[t] = (scale * sbuf[t].astype(jnp.float32)).astype(ubuf.dtype)

    def product(buf, r, off, height):
        count = counts[r, 0]
        value = None
        for s in range(slots):
            live = jnp.clip(count - s, 0, 1)
            block = buf[live * cols[r, s] + (1 - live) * col_tiles]
            left = tiles[r, s] if height == side else tiles[r, s, pl.ds(off, height)]
            term = jnp.dot(left, block, preferred_element_type=jnp.float32)
            value = term if value is None else value + term
        return value

    for t in range(col_tiles):
        psend[pl.ds(t * side, side)] = product(ubuf, (1 - c) * col_tiles + t, 0, side).astype(
            psend.dtype
        )
        remote(rows(psend, t), rows(precv, t), psd.at[t], prc.at[t], i, j + 1 - 2 * c).start()

    below = jnp.logical_and(z > 0, z <= i)
    above = jnp.logical_and(z < floors - 1, z >= i)
    sq[0] = jnp.zeros_like(sq[0])
    for t in range(col_tiles):
        acc[pl.ds(t * side, side)] = product(ubuf, c * col_tiles + t, 0, side)
    for t in range(col_tiles):
        here = pl.ds(t * side, side)
        wait(rows(precv, t), prc.at[t])
        acc[here] += precv[here].astype(jnp.float32)

        @pl.when(below)
        def _():
            wait(rows(clow, t), clr.at[t])
            acc[here] += clow[here].astype(jnp.float32)

        @pl.when(above)
        def _():
            wait(rows(chigh, t), chr_.at[t])
            acc[here] += chigh[here].astype(jnp.float32)

        @pl.when(jnp.logical_not(root))
        def _():
            csend[here] = acc[here].astype(csend.dtype)

        @pl.when(z < i)
        def _():
            remote(rows(csend, t), rows(clow, t), csd.at[t], clr.at[t], i, j + 2).start()

        @pl.when(z > i)
        def _():
            remote(rows(csend, t), rows(chigh, t), csd.at[t], chr_.at[t], i, j - 2).start()

        @pl.when(root)
        def _():
            mixed = scol[here] * (acc[here] + ubuf[t].astype(jnp.float32))
            vbuf[t] = (scol[here] * mixed).astype(vbuf.dtype)
            fan_out(vbuf, vsend, vrecv, t)
            sq[0, 0:1] += jnp.sum(mixed * mixed, axis=0, keepdims=True)

    for n in range(blocks):
        wait(deg_share.at[n], dsr.at[n])
    for t in range(share_tiles):
        degree = deg_share[0, t]
        for n in range(1, blocks):
            degree = degree + deg_share[n, t]
        sshare[pl.ds(t * side, side)] = jnp.broadcast_to(upright(degree)[:, :1], (side, width))

    @pl.when(jnp.logical_not(root))
    def _():
        for t in range(col_tiles):
            wait(rows(vbuf, t), vrecv.at[t])
            pass_on(vbuf, vsend, vrecv, t)

    def share_product(gy, put):
        for p in range(pieces):
            first = gy * share + p * piece
            off = pl.multiple_of(lax.rem(first, side), piece) if piece < side else 0
            value = product(vbuf, lax.div(first, side), off, piece)
            own = jnp.logical_and(root, lax.div(first, depth) == c)
            tile = lax.div(lax.rem(first, depth), side)
            block = vbuf[tile] if piece == side else vbuf[tile, pl.ds(off, piece)]
            put(p, value + jnp.where(own, block.astype(jnp.float32), 0.0))

    for n in range(1, floors + 1):
        floor = lax.rem(z + n, floors)

        def put(p, value):
            p2send[floor, pl.ds(p * piece, piece)] = value.astype(p2send.dtype)

        share_product(2 * floor + 1 - c, put)
        remote(
            p2send.at[floor], p2recv.at[floor], p2s.at[floor], p2r.at[floor], i, j + 1 - 2 * c
        ).start()

    for n in range(1, floors + 1):
        floor = lax.rem(z + n, floors)

        def put(p, value):
            last[pl.ds(p * piece, piece)] = value

        share_product(2 * floor + c, put)
        wait(p2recv.at[floor], p2r.at[floor])
        last[...] += p2recv[floor].astype(jnp.float32)
        if n < floors:
            r2send[floor] = last[...].astype(r2send.dtype)
            remote(
                r2send.at[floor], r2recv.at[z], r2s.at[floor], r2r.at[z], i, 2 * floor + c
            ).start()

    for n in range(1, floors):
        floor = lax.rem(z + n, floors)
        wait(r2recv.at[floor], r2r.at[floor])
        last[...] += r2recv[floor].astype(jnp.float32)

    if share < side:
        begin = pl.multiple_of(lax.rem(j * share, side), share)
        mixed = sshare[pl.ds(begin, share)] * last[...]
    else:
        mixed = sshare[...] * last[...]
    last[...] = mixed
    sq[0, 1:2] = jnp.sum(mixed * mixed, axis=0, keepdims=True)

    @pl.loop(1, total)
    def _(k):
        other = lax.rem(me + k, total)
        remote(
            sq.at[0],
            sq.at[total - k],
            qs,
            qr,
            lax.div(other, blocks),
            lax.rem(other, blocks),
        ).start()

    fan_done(sbuf, ssend)
    fan_done(vbuf, vsend)
    for h in range(2):
        source = rs.at[pl.ds(h * col_tiles, col_tiles)]
        for n in range(groups):
            if n > 0:
                wait(source, dcs.at[h * groups + n])
            else:

                @pl.when(2 * i + h != j)
                def _():
                    wait(source, dcs.at[h * groups + n])

    for n in range(1, blocks):
        wait(share_of(j), dss.at[n])
    for t in range(col_tiles):
        wait(rows(psend, t), psd.at[t])

    @pl.when(jnp.logical_not(root))
    def _():
        for t in range(col_tiles):
            wait(rows(csend, t), csd.at[t])

    for n in range(1, floors + 1):
        floor = lax.rem(z + n, floors)
        wait(p2send.at[floor], p2s.at[floor])
        if n < floors:
            wait(r2send.at[floor], r2s.at[floor])

    others = sq.at[pl.ds(1, total - 1)]
    wait(others, qs)
    wait(others, qr)
    sums = jnp.sum(sq[...], axis=0)
    first = jnp.sqrt(sums[0:1] / nodes + 1e-06)
    second = jnp.sqrt(sums[1:2] / (first * first) / nodes + 1e-06)
    sums_out[0:1] = first
    sums_out[1:2] = second
    out[...] = last[...] / (first * second)


def on_device(groups, blocks, tiles, tile_cols, row_counts, start_block):
    row_tiles, slots, side, _ = tiles.shape
    width = start_block.shape[1]
    local_rows = row_tiles * side
    depth = local_rows * groups // blocks
    col_tiles = depth // side
    share = local_rows // blocks
    share_tiles = max(1, share // side)
    floors = blocks // 2
    total = groups * blocks
    fan = 2 if groups == 4 else groups - 1
    bf16, f32 = jnp.bfloat16, jnp.float32
    vmem, dma = pltpu.VMEM, pltpu.SemaphoreType.DMA
    spec = pl.BlockSpec
    out, scales = pl.pallas_call(
        functools.partial(kernel, groups, blocks),
        out_shape=(
            jax.ShapeDtypeStruct((share, width), f32),
            jax.ShapeDtypeStruct((2, width), f32),
        ),
        in_specs=[
            spec(memory_space=pl.ANY),
            spec(memory_space=pl.ANY),
            spec(memory_space=pltpu.SMEM),
            spec(memory_space=pltpu.SMEM),
        ],
        out_specs=(spec(memory_space=pltpu.VMEM), spec(memory_space=pltpu.VMEM)),
        scratch_shapes=[
            vmem(tiles.shape, bf16),
            vmem((col_tiles, side, width), bf16),
            vmem((col_tiles + 1, side, width), bf16),
            vmem((col_tiles + 1, side, width), bf16),
            vmem((depth, width), f32),
            vmem((share_tiles * side, width), f32),
            vmem((row_tiles, 1, side), f32),
            vmem((blocks, col_tiles, 1, side), f32),
            vmem((blocks, share_tiles, 1, side), f32),
            vmem((depth, width), bf16),
            vmem((depth, width), bf16),
            vmem((depth, width), f32),
            vmem((depth, width), bf16),
            vmem((depth, width), bf16),
            vmem((depth, width), bf16),
            vmem((floors, share, width), bf16),
            vmem((floors, share, width), bf16),
            vmem((floors, share, width), bf16),
            vmem((floors, share, width), bf16),
            vmem((share, width), f32),
            vmem((total, 2, width), f32),
            dma((LOADS,)),
            dma((fan, col_tiles)),
            dma((col_tiles,)),
            dma((2 * groups,)),
            dma((blocks,)),
            dma((blocks,)),
            dma((blocks,)),
            dma((col_tiles,)),
            dma((col_tiles,)),
            dma((col_tiles,)),
            dma((col_tiles,)),
            dma((col_tiles,)),
            dma((fan, col_tiles)),
            dma((col_tiles,)),
            dma((floors,)),
            dma((floors,)),
            dma((floors,)),
            dma((floors,)),
            dma,
            dma,
        ],
        compiler_params=pltpu.CompilerParams(collective_id=0, has_side_effects=True),
    )(tiles, start_block, tile_cols, row_counts)
    return out.astype(bf16), scales


def solution(mesh):
    placed = (P("gx", "gy", None, None), P("gx", "gy"), P("gx", "gy"), P("gx", None))
    return jax.shard_map(
        functools.partial(on_device, mesh.shape["gx"], mesh.shape["gy"]),
        mesh=mesh,
        in_specs=placed,
        out_specs=(P(("gx", "gy"), None), P()),
        check_vma=False,
    )
```

```python
import functools
import jax
import jax.numpy as jnp
from jax import lax
from jax.experimental import pallas as pl
from jax.experimental.pallas import tpu as pltpu
from jax.sharding import PartitionSpec as P

MESH = pl.DeviceIdType.MESH
LOADS = 4
LAG = 4
LAG2 = 1


def wait(ref, sem):
    pltpu.make_async_copy(ref, ref, sem).wait()


def kernel(
    groups,
    blocks,
    tiles_hbm,
    start_hbm,
    cols,
    counts,
    out,
    sums_out,
    tiles,
    sbuf,
    ubuf,
    vbuf,
    scol,
    sshare,
    rs,
    deg_col,
    deg_share,
    psend,
    precv,
    acc,
    csend,
    clow,
    chigh,
    p2send,
    p2recv,
    r2send,
    r2recv,
    last,
    sq,
    tsem,
    ssend,
    srecv,
    dcs,
    dcr,
    dss,
    dsr,
    psd,
    prc,
    csd,
    clr,
    chr_,
    vsend,
    vrecv,
    p2s,
    p2r,
    r2s,
    r2r,
    qs,
    qr,
    gate,
):
    row_tiles, slots, side, _ = tiles.shape
    col_tiles, _, width = acc.shape
    depth = col_tiles * side
    share = out.shape[0]
    floors = blocks // 2
    total = groups * blocks
    piece = min(side, share)
    pieces = share // piece
    share_tiles = max(1, share // side)
    square = groups == 4

    i = lax.axis_index("gx")
    j = lax.axis_index("gy")
    z = lax.div(j, 2)
    c = lax.rem(j, 2)
    me = i * blocks + j
    root = i == z
    if square:
        x, y = lax.rem(i, 2), lax.div(i, 2)
        across_x = y * 2 + 1 - x
        across_y = (1 - y) * 2 + x
        off_x = x != lax.rem(z, 2)
        off_y = y != lax.div(z, 2)
        only_x = jnp.logical_and(off_x, jnp.logical_not(off_y))
        only_y = jnp.logical_and(off_y, jnp.logical_not(off_x))
        fan = 2
        halves = 2
    else:
        fan = groups - 1
        halves = 1
    chunks = col_tiles * halves
    height_of = side // halves

    def rows(ref, t):
        if len(ref.shape) == 3:
            return ref.at[t]
        return ref.at[pl.ds(t * side, side)]

    def remote(src, dst, send, recv, gx, gy):
        return pltpu.make_async_remote_copy(
            src_ref=src,
            dst_ref=dst,
            send_sem=send,
            recv_sem=recv,
            device_id=(gx, gy),
            device_id_type=MESH,
        )

    def bit(ref, t):
        return ref.at[t // halves, pl.ds(t % halves * height_of, height_of)]

    def fan_out(buf, send, recv, t, rows, only=None):
        for p in range(fan) if only is None else (only,):
            if square:
                target = (across_x, across_y)[p]
            else:
                target = lax.rem(i + p + 1, groups)
            remote(rows(buf, t), rows(buf, t), send.at[p, t], recv.at[t], target, j).start()

    def pass_on(buf, send, recv, t, rows):
        if square:
            cond, target = ((only_x, across_y), (only_y, across_x))[t % 2]

            @pl.when(cond)
            def _():
                remote(rows(buf, t), rows(buf, t), send.at[0, t], recv.at[t], target, j).start()

    def fan_done(buf, send, rows):
        amount = send.shape[1]

        @pl.when(root)
        def _():
            for t in range(amount):
                for p in range(fan):
                    wait(rows(buf, t), send.at[p, t])

        if square:
            for parity, cond in ((0, only_x), (1, only_y)):

                @pl.when(cond)
                def _():
                    for t in range(parity, amount, 2):
                        wait(rows(buf, t), send.at[0, t])

    step = row_tiles // LOADS
    loads = [
        pltpu.make_async_copy(
            tiles_hbm.at[pl.ds(n * step, step)], tiles.at[pl.ds(n * step, step)], tsem.at[n]
        )
        for n in range(LOADS)
    ]
    barrier = pltpu.get_barrier_semaphore()

    def greet(semaphore, gx, gy):
        pl.semaphore_signal(semaphore, inc=1, device_id=(gx, gy), device_id_type=MESH)

    for n in range(1, groups):
        greet(barrier, lax.rem(i + n, groups), j)
    for n in range(1, blocks):
        greet(barrier, i, lax.rem(j + n, blocks))

    @pl.when(root)
    def _():
        for t in range(col_tiles):
            pltpu.make_async_copy(
                start_hbm.at[pl.ds(c * depth + t * side, side)], rows(sbuf, t), srecv.at[t]
            ).start()

    for load in loads:
        load.start()
    ubuf[col_tiles] = jnp.zeros((side, width), ubuf.dtype)
    vbuf[col_tiles] = jnp.zeros((side, width), vbuf.dtype)
    pl.semaphore_wait(barrier, groups + blocks - 2)
    for n in range(1, groups):
        greet(gate, lax.rem(i + n, groups), j)

    @pl.when(root)
    def _():
        for t in range(col_tiles):
            wait(rows(sbuf, t), srecv.at[t])
        if square:
            for turn in range(2):
                for t in range(0, col_tiles, 2):
                    fan_out(sbuf, ssend, srecv, t + turn, rows, 0)
                    fan_out(sbuf, ssend, srecv, t + 1 - turn, rows, 1)
        else:
            for t in range(col_tiles):
                fan_out(sbuf, ssend, srecv, t, rows)

    ones = jnp.ones((8, side), jnp.bfloat16)
    for r in range(row_tiles):
        if r % step == 0:
            loads[r // step].wait()
        count = counts[0, r]
        row = jnp.zeros((8, side), jnp.float32)
        for s in range(slots):
            part = lax.dot_general(
                ones, tiles[r, s], (((1,), (1,)), ((), ())), preferred_element_type=jnp.float32
            )
            row = row + jnp.clip(count - s, 0, 1).astype(jnp.float32) * part
        rs[r] = row[0:1]

    pl.semaphore_wait(gate, groups - 1)
    for h in range(2):
        source = rs.at[pl.ds(h * col_tiles, col_tiles)]
        for n in range(groups):
            target = lax.rem(i + n, groups)
            gy = 2 * i + h
            slot = deg_col.at[j]
            mine = jnp.logical_and(n == 0, gy == j)

            @pl.when(jnp.logical_not(mine))
            def _():
                remote(source, slot, dcs.at[h * groups + n], dcr.at[j], target, gy).start()

            @pl.when(mine)
            def _():
                pltpu.make_async_copy(source, slot, dcr.at[j]).start()

    def share_of(gy):
        return rs.at[pl.ds(lax.div(gy * share, side), share_tiles)]

    for n in range(1, blocks):
        gy = lax.rem(j + n, blocks)
        remote(share_of(gy), deg_share.at[j], dss.at[n], dsr.at[j], i, gy).start()
    pltpu.make_async_copy(share_of(j), deg_share.at[j], dsr.at[j]).start()

    if square:
        for parity, cond in ((0, only_x), (1, only_y)):

            @pl.when(cond)
            def _():
                for t in range(parity, col_tiles, 2):
                    wait(rows(sbuf, t), srecv.at[t])
                    pass_on(sbuf, ssend, srecv, t, rows)

    for n in range(blocks):
        wait(deg_col.at[n], dcr.at[n])

    def upright(degree):
        scale = 1.0 / jnp.sqrt(1.0 + degree)
        return jnp.transpose(jnp.broadcast_to(scale, (side, side)))

    for t in range(col_tiles):
        degree = deg_col[0, t]
        for n in range(1, blocks):
            degree = degree + deg_col[n, t]
        scale = upright(degree)[:, :1]
        scol[t] = jnp.broadcast_to(scale, (side, width))

    for t in range(col_tiles):
        if square:
            done = jnp.logical_or(root, (only_x, only_y)[t % 2])
        else:
            done = root

        @pl.when(jnp.logical_not(done))
        def _():
            wait(rows(sbuf, t), srecv.at[t])

    for t in range(col_tiles):
        ubuf[t] = (scol[t] * sbuf[t].astype(jnp.float32)).astype(ubuf.dtype)

    def product(buf, r, off, height):
        count = counts[0, r]
        value = None
        for s in range(slots):
            live = jnp.clip(count - s, 0, 1)
            block = buf[live * cols[s, r] + (1 - live) * col_tiles]
            left = tiles[r, s] if height == side else tiles[r, s, pl.ds(off, height)]
            term = jnp.dot(left, block, preferred_element_type=jnp.float32)
            value = term if value is None else value + term
        return value

    below = jnp.logical_and(z > 0, z <= i)
    above = jnp.logical_and(z < floors - 1, z >= i)
    sq[0] = jnp.zeros_like(sq[0])

    def give(t):
        psend[t] = product(ubuf, (1 - c) * col_tiles + t, 0, side).astype(psend.dtype)
        remote(rows(psend, t), rows(precv, t), psd.at[t], prc.at[t], i, j + 1 - 2 * c).start()

    def combine(t):
        wait(rows(precv, t), prc.at[t])
        acc[t] += precv[t].astype(jnp.float32)
        for u in range(t * halves, (t + 1) * halves):
            advance(u)

    def advance(u):
        here = (u // halves, pl.ds(u % halves * height_of, height_of))

        @pl.when(below)
        def _():
            wait(bit(clow, u), clr.at[u])
            acc[here] += clow[here].astype(jnp.float32)

        @pl.when(above)
        def _():
            wait(bit(chigh, u), chr_.at[u])
            acc[here] += chigh[here].astype(jnp.float32)

        @pl.when(jnp.logical_not(root))
        def _():
            csend[here] = acc[here].astype(csend.dtype)

        @pl.when(z < i)
        def _():
            remote(bit(csend, u), bit(clow, u), csd.at[u], clr.at[u], i, j + 2).start()

        @pl.when(z > i)
        def _():
            remote(bit(csend, u), bit(chigh, u), csd.at[u], chr_.at[u], i, j - 2).start()

        @pl.when(root)
        def _():
            mixed = scol[here] * (acc[here] + ubuf[here].astype(jnp.float32))
            vbuf[here] = (scol[here] * mixed).astype(vbuf.dtype)
            fan_out(vbuf, vsend, vrecv, u, bit)
            sq[0, 0:1] += jnp.sum(mixed * mixed, axis=0, keepdims=True)

    for t in range(col_tiles + LAG):
        if t < col_tiles:
            give(t)
        if t >= LAG:
            acc[t - LAG] = product(ubuf, c * col_tiles + t - LAG, 0, side)
            combine(t - LAG)

    for n in range(blocks):
        wait(deg_share.at[n], dsr.at[n])
    for t in range(share_tiles):
        degree = deg_share[0, t]
        for n in range(1, blocks):
            degree = degree + deg_share[n, t]
        sshare[pl.ds(t * side, side)] = jnp.broadcast_to(upright(degree)[:, :1], (side, width))

    @pl.when(jnp.logical_not(root))
    def _():
        for t in range(chunks):
            wait(bit(vbuf, t), vrecv.at[t])
            pass_on(vbuf, vsend, vrecv, t, bit)

    def share_product(gy, put):
        for p in range(pieces):
            first = gy * share + p * piece
            off = pl.multiple_of(lax.rem(first, side), piece) if piece < side else 0
            value = product(vbuf, lax.div(first, side), off, piece)
            own = jnp.logical_and(root, lax.div(first, depth) == c)
            tile = lax.div(lax.rem(first, depth), side)
            block = vbuf[tile] if piece == side else vbuf[tile, pl.ds(off, piece)]
            put(p, value + jnp.where(own, block.astype(jnp.float32), 0.0))

    far = []
    for n in range(floors - 1):
        down = floors - 1 - n
        down = jnp.where(down <= z, down - 1, down)
        up = jnp.where(n >= z, n + 1, n)
        far.append(jnp.where(2 * z < floors, down, up))
    order = far + [z]

    def give2(floor):
        def put(p, value):
            p2send[floor, pl.ds(p * piece, piece)] = value.astype(p2send.dtype)

        share_product(2 * floor + 1 - c, put)
        remote(
            p2send.at[floor], p2recv.at[floor], p2s.at[floor], p2r.at[floor], i, j + 1 - 2 * c
        ).start()

    def combine2(n, floor):
        def put(p, value):
            last[pl.ds(p * piece, piece)] = value

        share_product(2 * floor + c, put)
        wait(p2recv.at[floor], p2r.at[floor])
        last[...] += p2recv[floor].astype(jnp.float32)
        if n < floors - 1:
            r2send[floor] = last[...].astype(r2send.dtype)
            remote(
                r2send.at[floor], r2recv.at[z], r2s.at[floor], r2r.at[z], i, 2 * floor + c
            ).start()

    for n in range(floors + LAG2):
        if n < floors:
            give2(order[n])
        if n >= LAG2:
            combine2(n - LAG2, order[n - LAG2])

    for n in range(1, floors):
        floor = lax.rem(z + n, floors)
        wait(r2recv.at[floor], r2r.at[floor])
        last[...] += r2recv[floor].astype(jnp.float32)

    if share < side:
        begin = pl.multiple_of(lax.rem(j * share, side), share)
        mixed = sshare[pl.ds(begin, share)] * last[...]
    else:
        mixed = sshare[...] * last[...]
    last[...] = mixed
    sq[0, 1:2] = jnp.sum(mixed * mixed, axis=0, keepdims=True)

    @pl.loop(1, total)
    def _(k):
        other = lax.rem(me + k, total)
        remote(
            sq.at[0],
            sq.at[total - k],
            qs,
            qr,
            lax.div(other, blocks),
            lax.rem(other, blocks),
        ).start()

    fan_done(sbuf, ssend, rows)
    fan_done(vbuf, vsend, bit)
    for h in range(2):
        source = rs.at[pl.ds(h * col_tiles, col_tiles)]
        for n in range(groups):
            if n > 0:
                wait(source, dcs.at[h * groups + n])
            else:

                @pl.when(2 * i + h != j)
                def _():
                    wait(source, dcs.at[h * groups + n])

    for n in range(1, blocks):
        wait(share_of(j), dss.at[n])
    for t in range(col_tiles):
        wait(rows(psend, t), psd.at[t])

    @pl.when(jnp.logical_not(root))
    def _():
        for t in range(chunks):
            wait(bit(csend, t), csd.at[t])

    for n in range(1, floors + 1):
        floor = lax.rem(z + n, floors)
        wait(p2send.at[floor], p2s.at[floor])
        if n < floors:
            wait(r2send.at[floor], r2s.at[floor])

    others = sq.at[pl.ds(1, total - 1)]
    wait(others, qs)
    wait(others, qr)
    sums_out[...] = jnp.sum(sq[...], axis=0)
    out[...] = last[...]


def finish(nodes, mixed, sums, vectors, scales):
    first = jnp.sqrt(sums[0:1] / nodes + 1e-06)
    second = jnp.sqrt(sums[1:2] / (first * first) / nodes + 1e-06)
    scales[0:1] = first
    scales[1:2] = second
    vectors[...] = (mixed[...] / (first * second)).astype(vectors.dtype)


def on_device(groups, blocks, tiles, tile_cols, row_counts, start_block):
    row_tiles, slots, side, _ = tiles.shape
    width = start_block.shape[1]
    local_rows = row_tiles * side
    depth = local_rows * groups // blocks
    col_tiles = depth // side
    share = local_rows // blocks
    share_tiles = max(1, share // side)
    floors = blocks // 2
    total = groups * blocks
    fan = 2 if groups == 4 else groups - 1
    chunks = col_tiles * (2 if groups == 4 else 1)
    bf16, f32 = jnp.bfloat16, jnp.float32
    vmem, dma = pltpu.VMEM, pltpu.SemaphoreType.DMA
    spec = pl.BlockSpec
    out, scales = pl.pallas_call(
        functools.partial(kernel, groups, blocks),
        out_shape=(
            jax.ShapeDtypeStruct((share, width), f32),
            jax.ShapeDtypeStruct((2, width), f32),
        ),
        in_specs=[
            spec(memory_space=pl.ANY),
            spec(memory_space=pl.ANY),
            spec(memory_space=pltpu.SMEM),
            spec(memory_space=pltpu.SMEM),
        ],
        out_specs=(spec(memory_space=pltpu.VMEM), spec(memory_space=pltpu.VMEM)),
        scratch_shapes=[
            vmem(tiles.shape, bf16),
            vmem((col_tiles, side, width), bf16),
            vmem((col_tiles + 1, side, width), bf16),
            vmem((col_tiles + 1, side, width), bf16),
            vmem((col_tiles, side, width), f32),
            vmem((share_tiles * side, width), f32),
            vmem((row_tiles, 1, side), f32),
            vmem((blocks, col_tiles, 1, side), f32),
            vmem((blocks, share_tiles, 1, side), f32),
            vmem((col_tiles, side, width), bf16),
            vmem((col_tiles, side, width), bf16),
            vmem((col_tiles, side, width), f32),
            vmem((col_tiles, side, width), bf16),
            vmem((col_tiles, side, width), bf16),
            vmem((col_tiles, side, width), bf16),
            vmem((floors, share, width), bf16),
            vmem((floors, share, width), bf16),
            vmem((floors, share, width), bf16),
            vmem((floors, share, width), bf16),
            vmem((share, width), f32),
            vmem((total, 2, width), f32),
            dma((LOADS,)),
            dma((fan, col_tiles)),
            dma((col_tiles,)),
            dma((2 * groups,)),
            dma((blocks,)),
            dma((blocks,)),
            dma((blocks,)),
            dma((col_tiles,)),
            dma((col_tiles,)),
            dma((chunks,)),
            dma((chunks,)),
            dma((chunks,)),
            dma((fan, chunks)),
            dma((chunks,)),
            dma((floors,)),
            dma((floors,)),
            dma((floors,)),
            dma((floors,)),
            dma,
            dma,
            pltpu.SemaphoreType.REGULAR,
        ],
        compiler_params=pltpu.CompilerParams(collective_id=0, has_side_effects=True),
    )(tiles, start_block, tile_cols.T, row_counts.T)
    return pl.pallas_call(
        functools.partial(finish, local_rows * groups),
        out_shape=(
            jax.ShapeDtypeStruct((share, width), bf16),
            jax.ShapeDtypeStruct((2, width), f32),
        ),
    )(out, scales)


def solution(mesh):
    placed = (P("gx", "gy", None, None), P("gx", "gy"), P("gx", "gy"), P("gx", None))
    return jax.shard_map(
        functools.partial(on_device, mesh.shape["gx"], mesh.shape["gy"]),
        mesh=mesh,
        in_specs=placed,
        out_specs=(P(("gx", "gy"), None), P()),
        check_vma=False,
    )
```

```python
import functools
import jax
import jax.numpy as jnp
from jax import lax
from jax.experimental import pallas as pl
from jax.experimental.pallas import tpu as pltpu
from jax.sharding import PartitionSpec as P

MESH = pl.DeviceIdType.MESH
LOADS = 4
LAG = 2
LAG2 = 1


def wait(ref, sem):
    pltpu.make_async_copy(ref, ref, sem).wait()


def kernel(
    groups,
    blocks,
    tiles_hbm,
    start_hbm,
    cols,
    counts,
    out,
    sums_out,
    tiles,
    sbuf,
    ubuf,
    vbuf,
    scol,
    sshare,
    rs,
    deg_col,
    deg_share,
    psend,
    precv,
    acc,
    csend,
    clow,
    chigh,
    p2send,
    p2recv,
    r2send,
    r2recv,
    last,
    sq,
    tsem,
    ssend,
    srecv,
    dcs,
    dcr,
    dss,
    dsr,
    psd,
    prc,
    csd,
    clr,
    chr_,
    vsend,
    vrecv,
    p2s,
    p2r,
    r2s,
    r2r,
    qs,
    qr,
    gate,
):
    row_tiles, slots, side, _ = tiles.shape
    col_tiles, _, width = acc.shape
    depth = col_tiles * side
    share = out.shape[0]
    floors = blocks // 2
    total = groups * blocks
    piece = min(side, share)
    pieces = share // piece
    share_tiles = max(1, share // side)
    square = groups == 4

    i = lax.axis_index("gx")
    j = lax.axis_index("gy")
    z = lax.div(j, 2)
    c = lax.rem(j, 2)
    root = i == z
    if square:
        x, y = lax.rem(i, 2), lax.div(i, 2)
        across_x = y * 2 + 1 - x
        across_y = (1 - y) * 2 + x
        off_x = x != lax.rem(z, 2)
        off_y = y != lax.div(z, 2)
        only_x = jnp.logical_and(off_x, jnp.logical_not(off_y))
        only_y = jnp.logical_and(off_y, jnp.logical_not(off_x))
        fan = 2
        halves = 2
    else:
        fan = groups - 1
        halves = 1
    chunks = col_tiles * halves
    height_of = side // halves

    def rows(ref, t):
        if len(ref.shape) == 3:
            return ref.at[t]
        return ref.at[pl.ds(t * side, side)]

    def remote(src, dst, send, recv, gx, gy):
        return pltpu.make_async_remote_copy(
            src_ref=src,
            dst_ref=dst,
            send_sem=send,
            recv_sem=recv,
            device_id=(gx, gy),
            device_id_type=MESH,
        )

    def bit(ref, t):
        return ref.at[t // halves, pl.ds(t % halves * height_of, height_of)]

    def fan_out(buf, send, recv, t, rows, only=None):
        for p in range(fan) if only is None else (only,):
            if square:
                target = (across_x, across_y)[p]
            else:
                target = lax.rem(i + p + 1, groups)
            remote(rows(buf, t), rows(buf, t), send.at[p, t], recv.at[t], target, j).start()

    def pass_on(buf, send, recv, t, rows):
        if square:
            cond, target = ((only_x, across_y), (only_y, across_x))[t % 2]

            @pl.when(cond)
            def _():
                remote(rows(buf, t), rows(buf, t), send.at[0, t], recv.at[t], target, j).start()

    def fan_done(buf, send, rows):
        amount = send.shape[1]

        @pl.when(root)
        def _():
            for t in range(amount):
                for p in range(fan):
                    wait(rows(buf, t), send.at[p, t])

        if square:
            for parity, cond in ((0, only_x), (1, only_y)):

                @pl.when(cond)
                def _():
                    for t in range(parity, amount, 2):
                        wait(rows(buf, t), send.at[0, t])

    step = row_tiles // LOADS
    loads = [
        pltpu.make_async_copy(
            tiles_hbm.at[pl.ds(n * step, step)], tiles.at[pl.ds(n * step, step)], tsem.at[n]
        )
        for n in range(LOADS)
    ]
    barrier = pltpu.get_barrier_semaphore()

    def greet(semaphore, gx, gy):
        pl.semaphore_signal(semaphore, inc=1, device_id=(gx, gy), device_id_type=MESH)

    for n in range(1, groups):
        greet(barrier, lax.rem(i + n, groups), j)
    for n in range(1, blocks):
        greet(barrier, i, lax.rem(j + n, blocks))

    @pl.when(root)
    def _():
        for t in range(col_tiles):
            pltpu.make_async_copy(
                start_hbm.at[pl.ds(c * depth + t * side, side)], rows(sbuf, t), srecv.at[t]
            ).start()

    for load in loads:
        load.start()
    ubuf[col_tiles] = jnp.zeros((side, width), ubuf.dtype)
    vbuf[col_tiles] = jnp.zeros((side, width), vbuf.dtype)
    pl.semaphore_wait(barrier, groups + blocks - 2)
    for n in range(1, groups):
        greet(gate, lax.rem(i + n, groups), j)

    @pl.when(root)
    def _():
        for t in range(col_tiles):
            wait(rows(sbuf, t), srecv.at[t])
        if square:
            for turn in range(2):
                for t in range(0, col_tiles, 2):
                    fan_out(sbuf, ssend, srecv, t + turn, rows, 0)
                    fan_out(sbuf, ssend, srecv, t + 1 - turn, rows, 1)
        else:
            for t in range(col_tiles):
                fan_out(sbuf, ssend, srecv, t, rows)

    ones = jnp.ones((8, side), jnp.bfloat16)
    for r in range(row_tiles):
        if r % step == 0:
            loads[r // step].wait()
        count = counts[0, r]
        row = jnp.zeros((8, side), jnp.float32)
        for s in range(slots):
            part = lax.dot_general(
                ones, tiles[r, s], (((1,), (1,)), ((), ())), preferred_element_type=jnp.float32
            )
            row = row + jnp.clip(count - s, 0, 1).astype(jnp.float32) * part
        rs[r] = row[0:1]

    pl.semaphore_wait(gate, groups - 1)
    for h in range(2):
        source = rs.at[pl.ds(h * col_tiles, col_tiles)]
        for n in range(groups):
            target = lax.rem(i + n, groups)
            gy = 2 * i + h
            slot = deg_col.at[j]
            mine = jnp.logical_and(n == 0, gy == j)

            @pl.when(jnp.logical_not(mine))
            def _():
                remote(source, slot, dcs.at[h * groups + n], dcr.at[j], target, gy).start()

            @pl.when(mine)
            def _():
                pltpu.make_async_copy(source, slot, dcr.at[j]).start()

    def share_of(gy):
        return rs.at[pl.ds(lax.div(gy * share, side), share_tiles)]

    for n in range(1, blocks):
        gy = lax.rem(j + n, blocks)
        remote(share_of(gy), deg_share.at[j], dss.at[n], dsr.at[j], i, gy).start()
    pltpu.make_async_copy(share_of(j), deg_share.at[j], dsr.at[j]).start()

    if square:
        for parity, cond in ((0, only_x), (1, only_y)):

            @pl.when(cond)
            def _():
                for t in range(parity, col_tiles, 2):
                    wait(rows(sbuf, t), srecv.at[t])
                    pass_on(sbuf, ssend, srecv, t, rows)

    for n in range(blocks):
        wait(deg_col.at[n], dcr.at[n])

    def upright(degree):
        scale = 1.0 / jnp.sqrt(1.0 + degree)
        return jnp.transpose(jnp.broadcast_to(scale, (side, side)))

    for t in range(col_tiles):
        degree = deg_col[0, t]
        for n in range(1, blocks):
            degree = degree + deg_col[n, t]
        scale = upright(degree)[:, :1]
        scol[t] = jnp.broadcast_to(scale, (side, width))

    for t in range(col_tiles):
        if square:
            done = jnp.logical_or(root, (only_x, only_y)[t % 2])
        else:
            done = root

        @pl.when(jnp.logical_not(done))
        def _():
            wait(rows(sbuf, t), srecv.at[t])

    for t in range(col_tiles):
        ubuf[t] = (scol[t] * sbuf[t].astype(jnp.float32)).astype(ubuf.dtype)

    def product(buf, r, off, height):
        count = counts[0, r]
        value = None
        for s in range(slots):
            live = jnp.clip(count - s, 0, 1)
            block = buf[live * cols[s, r] + (1 - live) * col_tiles]
            left = tiles[r, s] if height == side else tiles[r, s, pl.ds(off, height)]
            term = jnp.dot(left, block, preferred_element_type=jnp.float32)
            value = term if value is None else value + term
        return value

    below = jnp.logical_and(z > 0, z <= i)
    above = jnp.logical_and(z < floors - 1, z >= i)
    sq[0] = jnp.zeros_like(sq[0])

    def give(t):
        psend[t] = product(ubuf, (1 - c) * col_tiles + t, 0, side).astype(psend.dtype)
        remote(rows(psend, t), rows(precv, t), psd.at[t], prc.at[t], i, j + 1 - 2 * c).start()

    def combine(t):
        wait(rows(precv, t), prc.at[t])
        acc[t] += precv[t].astype(jnp.float32)
        for u in range(t * halves, (t + 1) * halves):
            advance(u)

    def advance(u):
        here = (u // halves, pl.ds(u % halves * height_of, height_of))

        @pl.when(below)
        def _():
            wait(bit(clow, u), clr.at[u])
            acc[here] += clow[here].astype(jnp.float32)

        @pl.when(above)
        def _():
            wait(bit(chigh, u), chr_.at[u])
            acc[here] += chigh[here].astype(jnp.float32)

        @pl.when(jnp.logical_not(root))
        def _():
            csend[here] = acc[here].astype(csend.dtype)

        @pl.when(z < i)
        def _():
            remote(bit(csend, u), bit(clow, u), csd.at[u], clr.at[u], i, j + 2).start()

        @pl.when(z > i)
        def _():
            remote(bit(csend, u), bit(chigh, u), csd.at[u], chr_.at[u], i, j - 2).start()

        @pl.when(root)
        def _():
            mixed = scol[here] * (acc[here] + ubuf[here].astype(jnp.float32))
            vbuf[here] = (scol[here] * mixed).astype(vbuf.dtype)
            fan_out(vbuf, vsend, vrecv, u, bit)
            sq[0, 0:1] += jnp.sum(mixed * mixed, axis=0, keepdims=True)

    for t in range(col_tiles + LAG):
        if t < col_tiles:
            give(t)
        if t >= LAG:
            acc[t - LAG] = product(ubuf, c * col_tiles + t - LAG, 0, side)
            combine(t - LAG)

    for n in range(blocks):
        wait(deg_share.at[n], dsr.at[n])
    for t in range(share_tiles):
        degree = deg_share[0, t]
        for n in range(1, blocks):
            degree = degree + deg_share[n, t]
        sshare[pl.ds(t * side, side)] = jnp.broadcast_to(upright(degree)[:, :1], (side, width))

    @pl.when(jnp.logical_not(root))
    def _():
        for t in range(chunks):
            wait(bit(vbuf, t), vrecv.at[t])
            pass_on(vbuf, vsend, vrecv, t, bit)

    def share_product(gy, put):
        for p in range(pieces):
            first = gy * share + p * piece
            off = pl.multiple_of(lax.rem(first, side), piece) if piece < side else 0
            value = product(vbuf, lax.div(first, side), off, piece)
            own = jnp.logical_and(root, lax.div(first, depth) == c)
            tile = lax.div(lax.rem(first, depth), side)
            block = vbuf[tile] if piece == side else vbuf[tile, pl.ds(off, piece)]
            put(p, value + jnp.where(own, block.astype(jnp.float32), 0.0))

    far = []
    for n in range(floors - 1):
        down = floors - 1 - n
        down = jnp.where(down <= z, down - 1, down)
        up = jnp.where(n >= z, n + 1, n)
        far.append(jnp.where(2 * z < floors, down, up))
    order = far + [z]

    def give2(floor):
        def put(p, value):
            p2send[floor, pl.ds(p * piece, piece)] = value.astype(p2send.dtype)

        share_product(2 * floor + 1 - c, put)
        remote(
            p2send.at[floor], p2recv.at[floor], p2s.at[floor], p2r.at[floor], i, j + 1 - 2 * c
        ).start()

    def combine2(n, floor):
        def put(p, value):
            last[pl.ds(p * piece, piece)] = value

        share_product(2 * floor + c, put)
        wait(p2recv.at[floor], p2r.at[floor])
        last[...] += p2recv[floor].astype(jnp.float32)
        if n < floors - 1:
            r2send[floor] = last[...].astype(r2send.dtype)
            remote(
                r2send.at[floor], r2recv.at[z], r2s.at[floor], r2r.at[z], i, 2 * floor + c
            ).start()

    for n in range(floors + LAG2):
        if n < floors:
            give2(order[n])
        if n >= LAG2:
            combine2(n - LAG2, order[n - LAG2])

    for n in range(1, floors):
        floor = lax.rem(z + n, floors)
        wait(r2recv.at[floor], r2r.at[floor])
        last[...] += r2recv[floor].astype(jnp.float32)

    if share < side:
        begin = pl.multiple_of(lax.rem(j * share, side), share)
        mixed = sshare[pl.ds(begin, share)] * last[...]
    else:
        mixed = sshare[...] * last[...]
    last[...] = mixed
    sq[0, 1:2] = jnp.sum(mixed * mixed, axis=0, keepdims=True)

    def tell(k, gx, gy):
        remote(sq.at[0], sq.at[k], qs, qr, gx, gy).start()

    if square:
        across = [lax.rem(i + n, groups) for n in range(groups)]
        along = [lax.rem(j + n, blocks) for n in range(blocks)]
        for k in range(total - 1, 0, -1):
            tell(k, across[k // blocks], along[k % blocks])
    else:

        @pl.loop(1, total)
        def _(k):
            gx, gy = lax.div(k, blocks), lax.rem(k, blocks)
            tell(k, lax.rem(i + gx, groups), lax.rem(j + gy, blocks))

    fan_done(sbuf, ssend, rows)
    fan_done(vbuf, vsend, bit)
    for h in range(2):
        source = rs.at[pl.ds(h * col_tiles, col_tiles)]
        for n in range(groups):
            if n > 0:
                wait(source, dcs.at[h * groups + n])
            else:

                @pl.when(2 * i + h != j)
                def _():
                    wait(source, dcs.at[h * groups + n])

    for n in range(1, blocks):
        wait(share_of(j), dss.at[n])
    for t in range(col_tiles):
        wait(rows(psend, t), psd.at[t])

    @pl.when(jnp.logical_not(root))
    def _():
        for t in range(chunks):
            wait(bit(csend, t), csd.at[t])

    for n in range(1, floors + 1):
        floor = lax.rem(z + n, floors)
        wait(p2send.at[floor], p2s.at[floor])
        if n < floors:
            wait(r2send.at[floor], r2s.at[floor])

    others = sq.at[pl.ds(1, total - 1)]
    wait(others, qs)
    wait(others, qr)
    sums_out[...] = jnp.sum(sq[...], axis=0)
    out[...] = last[...]


def finish(nodes, mixed, sums, vectors, scales):
    first = jnp.sqrt(sums[0:1] / nodes + 1e-06)
    second = jnp.sqrt(sums[1:2] / (first * first) / nodes + 1e-06)
    scales[0:1] = first
    scales[1:2] = second
    vectors[...] = (mixed[...] / (first * second)).astype(vectors.dtype)


def on_device(groups, blocks, tiles, tile_cols, row_counts, start_block):
    row_tiles, slots, side, _ = tiles.shape
    width = start_block.shape[1]
    local_rows = row_tiles * side
    depth = local_rows * groups // blocks
    col_tiles = depth // side
    share = local_rows // blocks
    share_tiles = max(1, share // side)
    floors = blocks // 2
    total = groups * blocks
    fan = 2 if groups == 4 else groups - 1
    chunks = col_tiles * (2 if groups == 4 else 1)
    bf16, f32 = jnp.bfloat16, jnp.float32
    vmem, dma = pltpu.VMEM, pltpu.SemaphoreType.DMA
    spec = pl.BlockSpec
    out, scales = pl.pallas_call(
        functools.partial(kernel, groups, blocks),
        out_shape=(
            jax.ShapeDtypeStruct((share, width), f32),
            jax.ShapeDtypeStruct((2, width), f32),
        ),
        in_specs=[
            spec(memory_space=pl.ANY),
            spec(memory_space=pl.ANY),
            spec(memory_space=pltpu.SMEM),
            spec(memory_space=pltpu.SMEM),
        ],
        out_specs=(spec(memory_space=pltpu.VMEM), spec(memory_space=pltpu.VMEM)),
        scratch_shapes=[
            vmem(tiles.shape, bf16),
            vmem((col_tiles, side, width), bf16),
            vmem((col_tiles + 1, side, width), bf16),
            vmem((col_tiles + 1, side, width), bf16),
            vmem((col_tiles, side, width), f32),
            vmem((share_tiles * side, width), f32),
            vmem((row_tiles, 1, side), f32),
            vmem((blocks, col_tiles, 1, side), f32),
            vmem((blocks, share_tiles, 1, side), f32),
            vmem((col_tiles, side, width), bf16),
            vmem((col_tiles, side, width), bf16),
            vmem((col_tiles, side, width), f32),
            vmem((col_tiles, side, width), bf16),
            vmem((col_tiles, side, width), bf16),
            vmem((col_tiles, side, width), bf16),
            vmem((floors, share, width), bf16),
            vmem((floors, share, width), bf16),
            vmem((floors, share, width), bf16),
            vmem((floors, share, width), bf16),
            vmem((share, width), f32),
            vmem((total, 2, width), f32),
            dma((LOADS,)),
            dma((fan, col_tiles)),
            dma((col_tiles,)),
            dma((2 * groups,)),
            dma((blocks,)),
            dma((blocks,)),
            dma((blocks,)),
            dma((col_tiles,)),
            dma((col_tiles,)),
            dma((chunks,)),
            dma((chunks,)),
            dma((chunks,)),
            dma((fan, chunks)),
            dma((chunks,)),
            dma((floors,)),
            dma((floors,)),
            dma((floors,)),
            dma((floors,)),
            dma,
            dma,
            pltpu.SemaphoreType.REGULAR,
        ],
        compiler_params=pltpu.CompilerParams(collective_id=0, has_side_effects=True),
    )(tiles, start_block, tile_cols.T, row_counts.T)
    return pl.pallas_call(
        functools.partial(finish, local_rows * groups),
        out_shape=(
            jax.ShapeDtypeStruct((share, width), bf16),
            jax.ShapeDtypeStruct((2, width), f32),
        ),
    )(out, scales)


def solution(mesh):
    placed = (P("gx", "gy", None, None), P("gx", "gy"), P("gx", "gy"), P("gx", None))
    return jax.shard_map(
        functools.partial(on_device, mesh.shape["gx"], mesh.shape["gy"]),
        mesh=mesh,
        in_specs=placed,
        out_specs=(P(("gx", "gy"), None), P()),
        check_vma=False,
    )
```
